32 devices in a mesh: blk: 8 (over z, x), rep: 4 (over y, core).
Axes of the slice: x: 2, y: 2, z: 4, core: 2. Of those that a mesh axis runs over, the one named last changes fastest.
Arguments:
- embeddings: float32 [16384, 768], P(('blk', 'rep')), may hold values from -6 to 6
- ranks: int32 [16384], replicated, may hold values from 0 to 16383, each once
Outputs:
- earlier_best: float32 [16384], P(('blk', 'rep'))
- later_best: float32 [16384], P(('blk', 'rep'))
The draws below stay inside these ranges and needn't reach their ends.
Inputs may be any that keep to these rules, and one draw needn't show every extreme that they name: ranks is a permutation of 0 .. 16383.
All inputs are finite; a program needn't handle non-finite values.
Results may differ from the reference program's by a relative error of at most 0.0012.
Values may be sent and summed in bfloat16 or wider, within the bound.
A program may use at most 64 MiB of HBM per device.

```python
import jax
import jax.numpy as jnp
from jax import lax

D = 768
STEPS = 3
BLOCK = 2048
N = 16384
N_BLK = 8


def levels(rng, shape, cuts, low, top_value):
    def one(position, blocks):
        steps = jax.random.uniform(jax.random.fold_in(jax.random.fold_in(rng, 6), position), (blocks,), jnp.float32, low / len(cuts), top_value / len(cuts))
        return jnp.repeat(jnp.exp(steps), shape[position] // blocks).reshape((-1,) + (1,) * (len(shape) - position - 1))

    level = one(*cuts[0])
    for cut in cuts[1:]:
        level = level * one(*cut)
    return level


def noise(own_key, shape, spread, reach, shards=(), held_as=jnp.bfloat16):
    array = spread * jax.random.normal(own_key, shape, jnp.float32)
    if shards:
        array = array * levels(own_key, shape, shards, -0.22, 0.18)
    return jnp.clip(array, -reach, reach).astype(held_as)


def setup_inputs(seed: int = 0) -> dict:
    arg_keys = jax.random.split(jax.random.key(seed), 3)
    embeddings = noise(arg_keys[0], (N, D), 1.0, 6.0, ((0, 32),), jnp.float32)
    ranks = jax.random.permutation(arg_keys[1], N).astype(jnp.int32)
    return dict(embeddings=embeddings, ranks=ranks)


def reference(embeddings, ranks):
    squares = lax.optimization_barrier(jnp.sum(embeddings * embeddings, axis=1, keepdims=True))
    unit = (embeddings * lax.rsqrt(squares + 1e-06)).astype(jnp.bfloat16).astype(jnp.float32)
    units = unit.reshape(N_BLK, BLOCK, D)
    ordered = ranks.reshape(N_BLK, BLOCK)

    def one_block(index):
        host = units[index]
        host_rank = ordered[index]
        row_best = jnp.full((BLOCK,), -1.0, jnp.float32)
        columns = []
        for offset in range(STEPS + 1):
            other = (index - offset) % N_BLK
            scores = jnp.dot(host, units[other].T, precision=lax.Precision.HIGHEST, preferred_element_type=jnp.float32)
            kept = jnp.where(ordered[other][None, :] < host_rank[:, None], scores, jnp.float32(-1.0))
            row_best = jnp.maximum(row_best, lax.optimization_barrier(jnp.max(kept, axis=1)))
            columns.append(lax.optimization_barrier(jnp.max(kept, axis=0)))
        return (row_best, jnp.stack(columns))
    row_best, column_best = lax.map(one_block, jnp.arange(N_BLK, dtype=jnp.int32))
    later = column_best[:, 0]
    for offset in range(1, STEPS + 1):
        later = jnp.maximum(later, jnp.roll(column_best[:, offset], -offset, axis=0))
    return (row_best.reshape(N), later.reshape(N))
```

```python
import functools

import jax
import jax.numpy as jnp
from jax import lax
from jax.experimental import pallas as pl
from jax.experimental.pallas import tpu as pltpu
from jax.sharding import PartitionSpec as P

STEPS = 3
CHUNKS = 4
MESH = pl.DeviceIdType.MESH


def kernel(
    blocks, copies, emb_ref, ranks_ref, early_ref, late_ref,
    host, visit, host_rank, visit_rank, row_acc, col_acc, col_in, row_out, row_in,
    z_send, x_send, y_send, core_send, two_send, one_send, relay_send, col_send, row_send,
    visit_recv, y_recv, core_recv, relay_recv, col_recv, row_recv,
):
    rows = emb_ref.shape[0]
    part = rows // CHUNKS
    b = lax.axis_index("blk")
    r = lax.axis_index("rep")
    odd = lax.rem(b, 2)
    even = odd == 0

    def blk(offset):
        return lax.rem(b + offset + blocks, blocks)

    core = r + 1 - 2 * lax.rem(r, 2)
    far = lax.rem(r + copies // 2, copies)
    far_core = lax.rem(core + copies // 2, copies)
    peers = (core, far, far_core)

    barrier = pltpu.get_barrier_semaphore()
    for offset in (1, 2, 3, -1, -2, -3):
        pl.semaphore_signal(barrier, inc=1, device_id=(blk(offset), r), device_id_type=MESH)
    for peer in peers:
        pl.semaphore_signal(barrier, inc=1, device_id=(b, peer), device_id_type=MESH)

    def normalise(i, _):
        at = pl.ds(pl.multiple_of(i * 64, 64), 64)
        x = emb_ref[at, :]
        squares = jnp.sum(x * x, axis=1, keepdims=True)
        host[0, at, :] = (x * lax.rsqrt(squares + 1e-06)).astype(jnp.bfloat16)
        return 0

    lax.fori_loop(0, rows // 64, normalise, 0)

    def cut(i):
        return pl.ds(pl.multiple_of(i * part, part), part)

    pl.semaphore_wait(barrier, 9)

    def send(src, dst, send_sem, recv_sem, device):
        copy = pltpu.make_async_remote_copy(
            src_ref=src, dst_ref=dst, send_sem=send_sem, recv_sem=recv_sem,
            device_id=device, device_id_type=MESH,
        )
        return copy

    def z_copy(i):
        return send(host.at[0, cut(i)], visit.at[1, cut(i)], z_send.at[i],
                    visit_recv.at[1, i], (blk(2), r))

    def x_copy(i):
        return send(host.at[0, cut(i)], visit.at[0, cut(i)], x_send.at[i],
                    visit_recv.at[0, i], (blk(1), r))

    def y_copy(i):
        return send(host.at[0, cut(i)], host.at[2, cut(i)], y_send.at[i],
                    y_recv.at[i], (b, far))

    def core_copy():
        return send(host.at[0], host.at[1], core_send, core_recv, (b, core))

    def relay_copy(i):
        return send(host.at[2, cut(i)], host.at[3, cut(i)], relay_send.at[i],
                    relay_recv.at[i], (b, core))

    def two_copy(i):
        slot = 2 - 2 * odd
        return send(visit.at[1, cut(i)], visit.at[slot, cut(i)], two_send.at[i],
                    visit_recv.at[slot, i], (blk(1 - 2 * odd), r))

    def one_copy(i):
        return send(visit.at[0, cut(i)], visit.at[2, cut(i)], one_send.at[i],
                    visit_recv.at[2, i], (blk(2), r))

    core_copy().start()
    for i in range(CHUNKS):
        z_copy(i).start()
        y_copy(i).start()

        @pl.when(even)
        def _():
            x_copy(i).start()

    owners = (r,) + peers
    for h, owner in enumerate(owners):
        line = ranks_ref[pl.ds(b * copies + owner, 1), :]
        host_rank[h] = jnp.broadcast_to(line, (128, rows)).T
    for slot, offset in enumerate((1, 2, 3, 0)):
        line = ranks_ref[pl.ds(blk(-offset) * copies + r, 1), :]
        visit_rank[slot] = jnp.broadcast_to(line, (8, rows))
    row_acc[...] = jnp.full(row_acc.shape, -1.0, jnp.float32)
    col_acc[...] = jnp.full(col_acc.shape, -1.0, jnp.float32)

    def score(other, slot, start, size, h):
        at = pl.ds(pl.multiple_of(start, size), size)
        scores = lax.dot_general(
            host[h], other[at, :], (((1,), (1,)), ((), ())),
            preferred_element_type=jnp.float32,
        )
        line = visit_rank[slot, 0:1, at]
        best = row_acc[h]
        for g in range(size // 128):
            kept = jnp.where(
                line[:, g * 128:(g + 1) * 128] < host_rank[h],
                scores[:, g * 128:(g + 1) * 128], jnp.float32(-1.0),
            )
            best = jnp.maximum(best, kept)
            column = jnp.max(kept.reshape(rows // 8, 8, 128), axis=0)
            there = pl.ds(pl.multiple_of(start + g * 128, 128), 128)
            col_acc[slot, :, there] = jnp.maximum(col_acc[slot, :, there], column)
        row_acc[h] = best

    wide = 256

    def sweep(other, slot, low, high):
        def step(t, _):
            h = low + t // (rows // wide)
            c = lax.rem(t, rows // wide)
            score(other, slot, c * wide, wide, h)
            return 0
        lax.fori_loop(0, (high - low) * (rows // wide), step, 0)

    sweep(host.at[0], 3, 0, 1)
    core_copy().wait_recv()
    sweep(host.at[0], 3, 1, 2)

    def arrive(i, _):
        y_copy(i).wait_recv()
        relay_copy(i).start()
        z_copy(i).wait_recv()
        two_copy(i).start()
        lax.fori_loop(0, 2, lambda h, c: (score(visit.at[1], 1, i * part, part, h), c)[1], 0)
        x_copy(i).wait_recv()

        @pl.when(even)
        def _():
            one_copy(i).start()

        lax.fori_loop(0, 2, lambda h, c: (score(visit.at[0], 0, i * part, part, h), c)[1], 0)
        return 0

    lax.fori_loop(0, CHUNKS, arrive, 0)
    for i in range(CHUNKS):
        relay_copy(i).wait_recv()
    sweep(host.at[0], 3, 2, 4)
    sweep(visit.at[1], 1, 2, 4)
    sweep(visit.at[0], 0, 2, 4)

    def col_copy(k):
        return send(col_acc.at[k], col_in.at[k], col_send.at[k], col_recv.at[k],
                    (blk(-1 - k), r))

    def last(i, _):
        one_copy(i).wait_recv()
        lax.fori_loop(0, 4, lambda h, c: (score(visit.at[2], 2, i * part, part, h), c)[1], 0)
        return 0

    col_copy(1).start()
    col_copy(0).start()
    lax.fori_loop(0, CHUNKS, last, 0)
    col_copy(2).start()

    def row_copy(k):
        return send(row_out.at[k], row_in.at[k], row_send.at[k], row_recv.at[k], (b, peers[k]))

    for k in range(3):
        best = jnp.max(row_acc[k + 1].T.reshape(16, 8, rows), axis=0)
        row_out[k] = best
        row_copy(k).start()

    early = jnp.max(row_acc[0].T.reshape(16, 8, rows), axis=0)
    late = col_acc[3]
    for k in range(3):
        row_copy(k).wait_recv()
        early = jnp.maximum(early, row_in[k])
    for k in range(3):
        col_copy(k).wait_recv()
        late = jnp.maximum(late, col_in[k])
    early_ref[...] = jnp.max(early, axis=0, keepdims=True)
    late_ref[...] = jnp.max(late, axis=0, keepdims=True)

    core_copy().wait_send()

    def drain(i, _):
        z_copy(i).wait_send()
        y_copy(i).wait_send()
        relay_copy(i).wait_send()
        two_copy(i).wait_send()

        @pl.when(even)
        def _():
            x_copy(i).wait_send()
            one_copy(i).wait_send()
        return 0

    lax.fori_loop(0, CHUNKS, drain, 0)
    for k in range(3):
        col_copy(k).wait_send()
        row_copy(k).wait_send()


def shards(embeddings, ranks):
    rows, width = embeddings.shape
    copies = lax.axis_size("rep")
    blocks = lax.axis_size("blk")
    lines = ranks.reshape(-1, rows)
    dma = pltpu.SemaphoreType.DMA
    vmem = pl.BlockSpec(memory_space=pltpu.VMEM)
    early, late = pl.pallas_call(
        functools.partial(kernel, blocks, copies),
        out_shape=[jax.ShapeDtypeStruct((1, rows), jnp.float32)] * 2,
        in_specs=[vmem, vmem],
        out_specs=[vmem, vmem],
        scratch_shapes=[
            pltpu.VMEM((4, rows, width), jnp.bfloat16),
            pltpu.VMEM((STEPS, rows, width), jnp.bfloat16),
            pltpu.VMEM((4, rows, 128), jnp.int32),
            pltpu.VMEM((4, 8, rows), jnp.int32),
            pltpu.VMEM((4, rows, 128), jnp.float32),
            pltpu.VMEM((4, 8, rows), jnp.float32),
            pltpu.VMEM((3, 8, rows), jnp.float32),
            pltpu.VMEM((3, 8, rows), jnp.float32),
            pltpu.VMEM((3, 8, rows), jnp.float32),
            dma((CHUNKS,)), dma((CHUNKS,)), dma((CHUNKS,)), dma,
            dma((CHUNKS,)), dma((CHUNKS,)), dma((CHUNKS,)), dma((3,)), dma((3,)),
            dma((STEPS, CHUNKS)), dma((CHUNKS,)), dma, dma((CHUNKS,)), dma((3,)), dma((3,)),
        ],
        compiler_params=pltpu.CompilerParams(
            collective_id=0, has_side_effects=True, vmem_limit_bytes=32 * 1024 * 1024
        ),
    )(embeddings, lines)
    return early.reshape(rows), late.reshape(rows)


def solution(mesh):
    return jax.shard_map(
        shards,
        mesh=mesh,
        in_specs=(P(("blk", "rep"), None), P()),
        out_specs=(P(("blk", "rep")), P(("blk", "rep"))),
        check_vma=False,
    )
```

```python
import functools

import jax
import jax.numpy as jnp
from jax import lax
from jax.experimental import pallas as pl
from jax.experimental.pallas import tpu as pltpu
from jax.sharding import PartitionSpec as P

STEPS = 3
CHUNKS = 4
MESH = pl.DeviceIdType.MESH


def kernel(
    blocks, copies, emb_ref, ranks_ref, early_ref, late_ref,
    emb, load_sem, host, visit, host_rank, visit_rank, row_acc, col_acc, col_in, row_out, row_in,
    z_send, x_send, y_send, core_send, two_send, one_send, relay_send, col_send, row_send,
    visit_recv, y_recv, core_recv, relay_recv, col_recv, row_recv,
):
    rows = emb_ref.shape[0]
    part = rows // CHUNKS
    b = lax.axis_index("blk")
    r = lax.axis_index("rep")
    odd = lax.rem(b, 2)
    even = odd == 0

    def blk(offset):
        return lax.rem(b + offset + blocks, blocks)

    core = r + 1 - 2 * lax.rem(r, 2)
    far = lax.rem(r + copies // 2, copies)
    far_core = lax.rem(core + copies // 2, copies)
    peers = (core, far, far_core)

    barrier = pltpu.get_barrier_semaphore()
    for offset in (1, 2, 3, -1, -2, -3):
        pl.semaphore_signal(barrier, inc=1, device_id=(blk(offset), r), device_id_type=MESH)
    for peer in peers:
        pl.semaphore_signal(barrier, inc=1, device_id=(b, peer), device_id_type=MESH)

    def cut(i):
        return pl.ds(pl.multiple_of(i * part, part), part)

    for i in range(CHUNKS):
        pltpu.make_async_copy(emb_ref.at[cut(i)], emb.at[cut(i)], load_sem.at[i]).start()

    def send(src, dst, send_sem, recv_sem, device):
        copy = pltpu.make_async_remote_copy(
            src_ref=src, dst_ref=dst, send_sem=send_sem, recv_sem=recv_sem,
            device_id=device, device_id_type=MESH,
        )
        return copy

    def z_copy(i):
        return send(host.at[0, cut(i)], visit.at[1, cut(i)], z_send.at[i],
                    visit_recv.at[1, i], (blk(2), r))

    def x_copy(i):
        return send(host.at[0, cut(i)], visit.at[0, cut(i)], x_send.at[i],
                    visit_recv.at[0, i], (blk(1), r))

    def y_copy(i):
        return send(host.at[0, cut(i)], host.at[2, cut(i)], y_send.at[i],
                    y_recv.at[i], (b, far))

    def core_copy():
        return send(host.at[0], host.at[1], core_send, core_recv, (b, core))

    def relay_copy(i):
        return send(host.at[2, cut(i)], host.at[3, cut(i)], relay_send.at[i],
                    relay_recv.at[i], (b, core))

    def two_copy(i):
        slot = 2 - 2 * odd
        return send(visit.at[1, cut(i)], visit.at[slot, cut(i)], two_send.at[i],
                    visit_recv.at[slot, i], (blk(1 - 2 * odd), r))

    def one_copy(i):
        return send(visit.at[0, cut(i)], visit.at[2, cut(i)], one_send.at[i],
                    visit_recv.at[2, i], (blk(2), r))

    def load(i):
        return pltpu.make_async_copy(emb_ref.at[cut(i)], emb.at[cut(i)], load_sem.at[i])

    def normalise(i):
        load(i).wait()
        for j in range(part // 32):
            at = pl.ds(i * part + j * 32, 32)
            x = emb[at, :]
            squares = jnp.sum(x * x, axis=1, keepdims=True)
            host[0, at, :] = (x * lax.rsqrt(squares + 1e-06)).astype(jnp.bfloat16)

    def spread(i):
        z_copy(i).start()
        y_copy(i).start()

        @pl.when(even)
        def _():
            x_copy(i).start()

    lines = rows // 128
    row_acc[...] = jnp.full(row_acc.shape, -1.0, jnp.float32)
    col_acc[...] = jnp.full(col_acc.shape, -1.0, jnp.float32)
    normalise(0)
    normalise(1)
    pl.semaphore_wait(barrier, 9)
    spread(0)
    for i in range(2, CHUNKS):
        normalise(i)
        spread(i - 1)
    for slot, offset in enumerate((1, 2, 3, 0)):
        for g in range(lines):
            line = ranks_ref[pl.ds((blk(-offset) * copies + r) * lines + g, 1), :]
            visit_rank[slot, :, g * 128:(g + 1) * 128] = jnp.broadcast_to(line, (8, 128))
    spread(CHUNKS - 1)
    core_copy().start()
    for h, owner in enumerate((r,) + peers):
        for g in range(lines):
            line = ranks_ref[pl.ds((b * copies + owner) * lines + g, 1), :]
            host_rank[h, g * 128:(g + 1) * 128, :] = jnp.broadcast_to(line, (128, 128)).T

    def score(other, slot, start, size, h):
        at = pl.ds(pl.multiple_of(start, size), size)
        scores = lax.dot_general(
            host[h], other[at, :], (((1,), (1,)), ((), ())),
            preferred_element_type=jnp.float32,
        )
        line = visit_rank[slot, 0:1, at]
        best = row_acc[h]
        for g in range(size // 128):
            kept = jnp.where(
                line[:, g * 128:(g + 1) * 128] < host_rank[h],
                scores[:, g * 128:(g + 1) * 128], jnp.float32(-1.0),
            )
            best = jnp.maximum(best, kept)
            column = jnp.max(kept.reshape(rows // 8, 8, 128), axis=0)
            there = pl.ds(pl.multiple_of(start + g * 128, 128), 128)
            col_acc[slot, :, there] = jnp.maximum(col_acc[slot, :, there], column)
        row_acc[h] = best

    wide = 256

    def sweep(other, slot, low, high):
        def step(t, _):
            h = low + t // (rows // wide)
            c = lax.rem(t, rows // wide)
            score(other, slot, c * wide, wide, h)
            return 0
        lax.fori_loop(0, (high - low) * (rows // wide), step, 0)

    sweep(host.at[0], 3, 0, 1)
    core_copy().wait_recv()
    sweep(host.at[0], 3, 1, 2)

    def arrive(i, _):
        y_copy(i).wait_recv()
        relay_copy(i).start()
        z_copy(i).wait_recv()
        two_copy(i).start()
        lax.fori_loop(0, 2, lambda h, c: (score(visit.at[1], 1, i * part, part, h), c)[1], 0)
        x_copy(i).wait_recv()

        @pl.when(even)
        def _():
            one_copy(i).start()

        lax.fori_loop(0, 2, lambda h, c: (score(visit.at[0], 0, i * part, part, h), c)[1], 0)
        return 0

    lax.fori_loop(0, CHUNKS, arrive, 0)
    for i in range(CHUNKS):
        relay_copy(i).wait_recv()
    sweep(host.at[0], 3, 2, 4)
    sweep(visit.at[1], 1, 2, 4)
    sweep(visit.at[0], 0, 2, 4)

    def col_copy(k):
        return send(col_acc.at[k], col_in.at[k], col_send.at[k], col_recv.at[k],
                    (blk(-1 - k), r))

    def last(i, _):
        one_copy(i).wait_recv()
        lax.fori_loop(0, 4, lambda h, c: (score(visit.at[2], 2, i * part, part, h), c)[1], 0)
        return 0

    col_copy(1).start()
    col_copy(0).start()
    lax.fori_loop(0, CHUNKS, last, 0)

    def row_copy(k):
        return send(row_out.at[k], row_in.at[k], row_send.at[k], row_recv.at[k], (b, peers[k]))

    for k in range(3):
        best = jnp.max(row_acc[k + 1].T.reshape(16, 8, rows), axis=0)
        row_out[k] = best

    col_copy(2).start()
    for k in range(3):
        row_copy(k).start()
    early = jnp.max(row_acc[0].T.reshape(16, 8, rows), axis=0)
    late = col_acc[3]
    for k in range(3):
        row_copy(k).wait_recv()
        early = jnp.maximum(early, row_in[k])
    for k in range(3):
        col_copy(k).wait_recv()
        late = jnp.maximum(late, col_in[k])
    early_ref[...] = jnp.max(early, axis=0, keepdims=True)
    late_ref[...] = jnp.max(late, axis=0, keepdims=True)

    core_copy().wait_send()

    def drain(i, _):
        z_copy(i).wait_send()
        y_copy(i).wait_send()
        relay_copy(i).wait_send()
        two_copy(i).wait_send()

        @pl.when(even)
        def _():
            x_copy(i).wait_send()
            one_copy(i).wait_send()
        return 0

    lax.fori_loop(0, CHUNKS, drain, 0)
    for k in range(3):
        col_copy(k).wait_send()
        row_copy(k).wait_send()


def shards(embeddings, ranks):
    rows, width = embeddings.shape
    copies = lax.axis_size("rep")
    blocks = lax.axis_size("blk")
    lines = ranks.reshape(-1, 128)
    dma = pltpu.SemaphoreType.DMA
    vmem = pl.BlockSpec(memory_space=pltpu.VMEM)
    early, late = pl.pallas_call(
        functools.partial(kernel, blocks, copies),
        out_shape=[jax.ShapeDtypeStruct((1, rows), jnp.float32)] * 2,
        in_specs=[pl.BlockSpec(memory_space=pltpu.HBM), vmem],
        out_specs=[vmem, vmem],
        scratch_shapes=[
            pltpu.VMEM((rows, width), jnp.float32),
            dma((CHUNKS,)),
            pltpu.VMEM((4, rows, width), jnp.bfloat16),
            pltpu.VMEM((STEPS, rows, width), jnp.bfloat16),
            pltpu.VMEM((4, rows, 128), jnp.int32),
            pltpu.VMEM((4, 8, rows), jnp.int32),
            pltpu.VMEM((4, rows, 128), jnp.float32),
            pltpu.VMEM((4, 8, rows), jnp.float32),
            pltpu.VMEM((3, 8, rows), jnp.float32),
            pltpu.VMEM((3, 8, rows), jnp.float32),
            pltpu.VMEM((3, 8, rows), jnp.float32),
            dma((CHUNKS,)), dma((CHUNKS,)), dma((CHUNKS,)), dma,
            dma((CHUNKS,)), dma((CHUNKS,)), dma((CHUNKS,)), dma((3,)), dma((3,)),
            dma((STEPS, CHUNKS)), dma((CHUNKS,)), dma, dma((CHUNKS,)), dma((3,)), dma((3,)),
        ],
        compiler_params=pltpu.CompilerParams(
            collective_id=0, has_side_effects=True, vmem_limit_bytes=56 * 1024 * 1024
        ),
    )(embeddings, lines)
    return early.reshape(rows), late.reshape(rows)


def solution(mesh):
    return jax.shard_map(
        shards,
        mesh=mesh,
        in_specs=(P(("blk", "rep"), None), P()),
        out_specs=(P(("blk", "rep")), P(("blk", "rep"))),
        check_vma=False,
    )
```

```python
import functools

import jax
import jax.numpy as jnp
from jax import lax
from jax.experimental import pallas as pl
from jax.experimental.pallas import tpu as pltpu
from jax.sharding import PartitionSpec as P

STEPS = 3
CHUNKS = 4
MESH = pl.DeviceIdType.MESH


def kernel(
    blocks, copies, emb_ref, ranks_ref, early_ref, late_ref,
    emb, load_sem, host, visit, host_rank, visit_rank, row_acc, col_acc, col_in, row_out, row_in,
    z_send, x_send, y_send, core_send, two_send, one_send, relay_send, col_send, row_send,
    visit_recv, y_recv, core_recv, relay_recv, col_recv, row_recv,
):
    rows = emb_ref.shape[0]
    part = rows // CHUNKS
    b = lax.axis_index("blk")
    r = lax.axis_index("rep")
    odd = lax.rem(b, 2)
    even = odd == 0

    def blk(offset):
        return lax.rem(b + offset + blocks, blocks)

    core = r + 1 - 2 * lax.rem(r, 2)
    far = lax.rem(r + copies // 2, copies)
    far_core = lax.rem(core + copies // 2, copies)
    peers = (core, far, far_core)

    barrier = pltpu.get_barrier_semaphore()
    for other in (blk(2), blk(-2), b + 1 - 2 * odd):
        pl.semaphore_signal(barrier, inc=1, device_id=(other, r), device_id_type=MESH)
    for peer in peers:
        pl.semaphore_signal(barrier, inc=1, device_id=(b, peer), device_id_type=MESH)

    def cut(i):
        return pl.ds(pl.multiple_of(i * part, part), part)

    for i in range(CHUNKS):
        pltpu.make_async_copy(emb_ref.at[cut(i)], emb.at[cut(i)], load_sem.at[i]).start()

    def send(src, dst, send_sem, recv_sem, device):
        copy = pltpu.make_async_remote_copy(
            src_ref=src, dst_ref=dst, send_sem=send_sem, recv_sem=recv_sem,
            device_id=device, device_id_type=MESH,
        )
        return copy

    def z_copy(i):
        return send(host.at[0, cut(i)], visit.at[1, cut(i)], z_send.at[i],
                    visit_recv.at[1, i], (blk(2), r))

    def x_copy(i):
        return send(host.at[0, cut(i)], visit.at[0, cut(i)], x_send.at[i],
                    visit_recv.at[0, i], (blk(1), r))

    def y_copy(i):
        return send(host.at[0, cut(i)], host.at[2, cut(i)], y_send.at[i],
                    y_recv.at[i], (b, far))

    def core_copy():
        return send(host.at[0], host.at[1], core_send, core_recv, (b, core))

    def relay_copy(i):
        return send(host.at[2, cut(i)], host.at[3, cut(i)], relay_send.at[i],
                    relay_recv.at[i], (b, core))

    def two_copy(i):
        slot = 2 - 2 * odd
        return send(visit.at[1, cut(i)], visit.at[slot, cut(i)], two_send.at[i],
                    visit_recv.at[slot, i], (blk(1 - 2 * odd), r))

    def one_copy(i):
        return send(visit.at[0, cut(i)], visit.at[2, cut(i)], one_send.at[i],
                    visit_recv.at[2, i], (blk(2), r))

    def load(i):
        return pltpu.make_async_copy(emb_ref.at[cut(i)], emb.at[cut(i)], load_sem.at[i])

    def normalise(i):
        load(i).wait()
        for j in range(part // 32):
            at = pl.ds(i * part + j * 32, 32)
            x = emb[at, :]
            squares = jnp.sum(x * x, axis=1, keepdims=True)
            host[0, at, :] = (x * lax.rsqrt(squares + 1e-06)).astype(jnp.bfloat16)

    def spread(i):
        z_copy(i).start()
        y_copy(i).start()

        @pl.when(even)
        def _():
            x_copy(i).start()

    lines = rows // 128
    row_acc[...] = jnp.full(row_acc.shape, -1.0, jnp.float32)
    col_acc[...] = jnp.full(col_acc.shape, -1.0, jnp.float32)
    normalise(0)
    normalise(1)
    pl.semaphore_wait(barrier, 6)
    spread(0)
    for i in range(2, CHUNKS):
        normalise(i)
        spread(i - 1)
    for slot, offset in enumerate((1, 2, 3, 0)):
        for g in range(lines):
            line = ranks_ref[pl.ds((blk(-offset) * copies + r) * lines + g, 1), :]
            visit_rank[slot, :, g * 128:(g + 1) * 128] = jnp.broadcast_to(line, (8, 128))
    spread(CHUNKS - 1)
    core_copy().start()
    for h, owner in enumerate((r,) + peers):
        for g in range(lines):
            line = ranks_ref[pl.ds((b * copies + owner) * lines + g, 1), :]
            host_rank[h, g * 128:(g + 1) * 128, :] = jnp.broadcast_to(line, (128, 128)).T

    def score(other, slot, start, size, low, high):
        at = pl.ds(pl.multiple_of(start, size), size)
        span = (high - low) * rows
        scores = lax.dot_general(
            host[low:high].reshape(span, host.shape[2]), other[at, :], (((1,), (1,)), ((), ())),
            preferred_element_type=jnp.float32,
        )
        line = visit_rank[slot, 0:1, at]
        marks = host_rank[low:high].reshape(span, 128)
        best = row_acc[low:high].reshape(span, 128)
        for g in range(size // 128):
            kept = jnp.where(
                line[:, g * 128:(g + 1) * 128] < marks,
                scores[:, g * 128:(g + 1) * 128], jnp.float32(-1.0),
            )
            best = jnp.maximum(best, kept)
            column = jnp.max(kept.reshape(span // 8, 8, 128), axis=0)
            there = pl.ds(pl.multiple_of(start + g * 128, 128), 128)
            col_acc[slot, :, there] = jnp.maximum(col_acc[slot, :, there], column)
        row_acc[low:high] = best.reshape(high - low, rows, 128)

    wide = 256

    def sweep(other, slot, low, high):
        def step(c, _):
            score(other, slot, c * wide, wide, low, high)
            return 0
        lax.fori_loop(0, rows // wide, step, 0)

    sweep(host.at[0], 3, 0, 1)
    core_copy().wait_recv()
    sweep(host.at[0], 3, 1, 2)

    def arrive(i, _):
        y_copy(i).wait_recv()
        relay_copy(i).start()
        z_copy(i).wait_recv()
        two_copy(i).start()
        score(visit.at[1], 1, i * part, part, 0, 2)
        x_copy(i).wait_recv()

        @pl.when(even)
        def _():
            one_copy(i).start()

        score(visit.at[0], 0, i * part, part, 0, 2)
        return 0

    lax.fori_loop(0, CHUNKS, arrive, 0)
    for i in range(CHUNKS):
        relay_copy(i).wait_recv()
    sweep(host.at[0], 3, 2, 4)
    sweep(visit.at[1], 1, 2, 4)
    sweep(visit.at[0], 0, 2, 4)

    def col_copy(k):
        return send(col_acc.at[k], col_in.at[k], col_send.at[k], col_recv.at[k],
                    (blk(-1 - k), r))

    def last(i, _):
        one_copy(i).wait_recv()
        score(visit.at[2], 2, i * part, part, 0, 4)
        return 0

    col_copy(1).start()
    col_copy(0).start()
    lax.fori_loop(0, CHUNKS, last, 0)

    def row_copy(k):
        return send(row_out.at[k], row_in.at[k], row_send.at[k], row_recv.at[k], (b, peers[k]))

    for k in range(3):
        best = jnp.max(row_acc[k + 1].T.reshape(16, 8, rows), axis=0)
        row_out[k] = best

    col_copy(2).start()
    for k in range(3):
        row_copy(k).start()
    early = jnp.max(row_acc[0].T.reshape(16, 8, rows), axis=0)
    late = col_acc[3]
    for k in range(3):
        row_copy(k).wait_recv()
        early = jnp.maximum(early, row_in[k])
    for k in range(3):
        col_copy(k).wait_recv()
        late = jnp.maximum(late, col_in[k])
    early_ref[...] = jnp.max(early, axis=0, keepdims=True)
    late_ref[...] = jnp.max(late, axis=0, keepdims=True)

    core_copy().wait_send()

    def drain(i, _):
        z_copy(i).wait_send()
        y_copy(i).wait_send()
        relay_copy(i).wait_send()
        two_copy(i).wait_send()

        @pl.when(even)
        def _():
            x_copy(i).wait_send()
            one_copy(i).wait_send()
        return 0

    lax.fori_loop(0, CHUNKS, drain, 0)
    for k in range(3):
        col_copy(k).wait_send()
        row_copy(k).wait_send()


def shards(embeddings, ranks):
    rows, width = embeddings.shape
    copies = lax.axis_size("rep")
    blocks = lax.axis_size("blk")
    lines = ranks.reshape(-1, 128)
    dma = pltpu.SemaphoreType.DMA
    vmem = pl.BlockSpec(memory_space=pltpu.VMEM)
    early, late = pl.pallas_call(
        functools.partial(kernel, blocks, copies),
        out_shape=[jax.ShapeDtypeStruct((1, rows), jnp.float32)] * 2,
        in_specs=[pl.BlockSpec(memory_space=pltpu.HBM), vmem],
        out_specs=[vmem, vmem],
        scratch_shapes=[
            pltpu.VMEM((rows, width), jnp.float32),
            dma((CHUNKS,)),
            pltpu.VMEM((4, rows, width), jnp.bfloat16),
            pltpu.VMEM((STEPS, rows, width), jnp.bfloat16),
            pltpu.VMEM((4, rows, 128), jnp.int32),
            pltpu.VMEM((4, 8, rows), jnp.int32),
            pltpu.VMEM((4, rows, 128), jnp.float32),
            pltpu.VMEM((4, 8, rows), jnp.float32),
            pltpu.VMEM((3, 8, rows), jnp.float32),
            pltpu.VMEM((3, 8, rows), jnp.float32),
            pltpu.VMEM((3, 8, rows), jnp.float32),
            dma((CHUNKS,)), dma((CHUNKS,)), dma((CHUNKS,)), dma,
            dma((CHUNKS,)), dma((CHUNKS,)), dma((CHUNKS,)), dma((3,)), dma((3,)),
            dma((STEPS, CHUNKS)), dma((CHUNKS,)), dma, dma((CHUNKS,)), dma((3,)), dma((3,)),
        ],
        compiler_params=pltpu.CompilerParams(
            collective_id=0, has_side_effects=True, vmem_limit_bytes=63 * 1024 * 1024
        ),
    )(embeddings, lines)
    return early.reshape(rows), late.reshape(rows)


def solution(mesh):
    return jax.shard_map(
        shards,
        mesh=mesh,
        in_specs=(P(("blk", "rep"), None), P()),
        out_specs=(P(("blk", "rep")), P(("blk", "rep"))),
        check_vma=False,
    )
```

```python
import functools

import jax
import jax.numpy as jnp
from jax import lax
from jax.experimental import pallas as pl
from jax.experimental.pallas import tpu as pltpu
from jax.sharding import PartitionSpec as P

CHUNKS = 4
MESH = pl.DeviceIdType.MESH


def kernel(
    blocks, copies, emb_ref, ranks_ref, early_ref, late_ref,
    emb, load_sem, host, visit, host_rank, visit_rank, row_acc, col_acc, col_in, row_out, row_in,
    z_send, x_send, y_send, core_send, relay_send, side_send, on_send, col_send, row_send,
    visit_recv, x_recv, y_recv, core_recv, relay_recv, col_recv, row_recv,
):
    rows = emb_ref.shape[0]
    part = rows // CHUNKS
    b = lax.axis_index("blk")
    r = lax.axis_index("rep")
    odd = lax.rem(b, 2)
    even = odd == 0

    def blk(offset):
        return lax.rem(b + offset + blocks, blocks)

    core = r + 1 - 2 * lax.rem(r, 2)
    far = lax.rem(r + copies // 2, copies)
    far_core = lax.rem(core + copies // 2, copies)
    peers = (core, far, far_core)

    barrier = pltpu.get_barrier_semaphore()
    for other in (blk(2), blk(-2), b + 1 - 2 * odd):
        pl.semaphore_signal(barrier, inc=1, device_id=(other, r), device_id_type=MESH)
    for peer in peers:
        pl.semaphore_signal(barrier, inc=1, device_id=(b, peer), device_id_type=MESH)

    def cut(i):
        return pl.ds(pl.multiple_of(i * part, part), part)

    for i in range(CHUNKS):
        pltpu.make_async_copy(emb_ref.at[cut(i)], emb.at[cut(i)], load_sem.at[i]).start()

    def send(src, dst, send_sem, recv_sem, device):
        copy = pltpu.make_async_remote_copy(
            src_ref=src, dst_ref=dst, send_sem=send_sem, recv_sem=recv_sem,
            device_id=device, device_id_type=MESH,
        )
        return copy

    def hrow(h, i):
        return pl.ds(pl.multiple_of(h * rows + i * part, part), part)

    keep = CHUNKS - 1
    across = b + 1 - 2 * odd

    def z_copy(i):
        return send(host.at[hrow(0, i)], visit.at[0, cut(i)], z_send.at[i],
                    visit_recv.at[0, i], (blk(2), r))

    def x_copy(i):
        return send(host.at[hrow(0, i)], host.at[hrow(4, i)], x_send.at[i],
                    x_recv.at[i], (across, r))

    def y_copy(i):
        return send(host.at[hrow(0, i)], host.at[hrow(2, i)], y_send.at[i],
                    y_recv.at[i], (b, far))

    def core_copy():
        return send(host.at[pl.ds(0, rows)], host.at[pl.ds(rows, rows)], core_send, core_recv,
                    (b, core))

    def relay_y(i):
        return send(host.at[hrow(2, i)], host.at[hrow(3, i)], relay_send.at[0, i],
                    relay_recv.at[0, i], (b, core))

    def relay_x(i):
        return send(host.at[hrow(4, i)], host.at[hrow(5, i)], relay_send.at[1, i],
                    relay_recv.at[1, i], (b, core))

    def side_copy(i):
        return send(visit.at[0, cut(i)], visit.at[1, cut(i)], side_send.at[i],
                    visit_recv.at[1, i], (across, r))

    def up_copy():
        return send(visit.at[0, cut(keep)], visit.at[2, cut(keep)], side_send.at[keep],
                    visit_recv.at[2, keep], (b, far))

    def on_copy(i):
        return send(visit.at[1, cut(i)], visit.at[3, cut(i)], on_send.at[i],
                    visit_recv.at[3, i], (blk(2), r))

    def on_v():
        return send(visit.at[0, cut(keep)], visit.at[3, cut(keep)], on_send.at[keep],
                    visit_recv.at[3, keep], (blk(2), r))

    def on_y():
        return send(visit.at[2, cut(keep)], visit.at[4, cut(keep)], on_send.at[keep + 1],
                    visit_recv.at[4, keep], (blk(2), r))

    def load(i):
        return pltpu.make_async_copy(emb_ref.at[cut(i)], emb.at[cut(i)], load_sem.at[i])

    def normalise(i):
        load(i).wait()
        for j in range(part // 32):
            at = pl.ds(i * part + j * 32, 32)
            x = emb[at, :]
            squares = jnp.sum(x * x, axis=1, keepdims=True)
            host[at, :] = (x * lax.rsqrt(squares + 1e-06)).astype(jnp.bfloat16)

    def spread(i):
        z_copy(i).start()
        y_copy(i).start()
        if i < 2:
            x_copy(i).start()

    lines = rows // 128
    row_acc[...] = jnp.full(row_acc.shape, -1.0, jnp.float32)
    col_acc[...] = jnp.full(col_acc.shape, -1.0, jnp.float32)
    normalise(0)
    normalise(1)
    pl.semaphore_wait(barrier, 6)
    spread(0)
    for i in range(2, CHUNKS):
        normalise(i)
        spread(i - 1)
    owners = (
        (blk(-2), r), (blk(-1 - 2 * odd), r), (blk(-2), far), (b, r),
        (blk(-3 + 2 * odd), r), (blk(-4), r), (blk(-4), far),
    )
    for slot, (block, rep) in enumerate(owners):
        for g in range(lines):
            line = ranks_ref[pl.ds((block * copies + rep) * lines + g, 1), :]
            visit_rank[slot, :, g * 128:(g + 1) * 128] = jnp.broadcast_to(line, (8, 128))
    spread(CHUNKS - 1)
    core_copy().start()
    row_owners = ((b, r), (b, core), (b, far), (b, far_core), (across, r), (across, core))
    for h, (block, rep) in enumerate(row_owners):
        for g in range(lines):
            line = ranks_ref[pl.ds((block * copies + rep) * lines + g, 1), :]
            host_rank[h * rows + g * 128:h * rows + (g + 1) * 128, :] = jnp.broadcast_to(line, (128, 128)).T

    def score(other, slot, start, size, low, span):
        at = pl.ds(pl.multiple_of(start, size), size)
        mine = pl.ds(low, span)
        scores = lax.dot_general(
            host[mine, :], other[at, :], (((1,), (1,)), ((), ())),
            preferred_element_type=jnp.float32,
        )
        line = visit_rank[slot, 0:1, at]
        marks = host_rank[mine, :]
        best = row_acc[mine, :]
        for g in range(size // 128):
            kept = jnp.where(
                line[:, g * 128:(g + 1) * 128] < marks,
                scores[:, g * 128:(g + 1) * 128], jnp.float32(-1.0),
            )
            best = jnp.maximum(best, kept)
            column = jnp.max(kept.reshape(span // 8, 8, 128), axis=0)
            there = pl.ds(pl.multiple_of(start + g * 128, 128), 128)
            col_acc[slot, :, there] = jnp.maximum(col_acc[slot, :, there], column)
        row_acc[mine, :] = best

    wide = 256

    def sweep(other, slot, low, span):
        def step(c, _):
            score(other, slot, c * wide, wide, low, span)
            return 0
        lax.fori_loop(0, rows // wide, step, 0)

    own = host.at[pl.ds(0, rows)]
    beside = host.at[pl.ds(4 * rows, rows)]
    sweep(own, 3, 0, rows)
    core_copy().wait_recv()
    sweep(own, 3, rows, rows)

    for i in range(CHUNKS):
        y_copy(i).wait_recv()
        relay_y(i).start()
        z_copy(i).wait_recv()
        if i < keep:
            side_copy(i).start()
            if i == keep - 1:
                for j in range(2, CHUNKS):
                    x_copy(j).start()
        else:
            up_copy().start()

            @pl.when(odd == 1)
            def _():
                on_v().start()
        if i < 2:
            x_copy(i).wait_recv()
            relay_x(i).start()
        score(visit.at[0], 0, i * part, part, 0, 2 * rows)

    def onward(i):
        side_copy(i).wait_recv()

        @pl.when(even)
        def _():
            on_copy(i).start()

    for i in range(keep - 1):
        onward(i)
    for i in range(CHUNKS):
        relay_y(i).wait_recv()
    sweep(own, 3, 2 * rows, 2 * rows)
    onward(keep - 1)
    up_copy().wait_recv()

    @pl.when(odd == 1)
    def _():
        on_y().start()

    sweep(visit.at[0], 0, 2 * rows, 2 * rows)
    for i in range(keep):
        score(visit.at[1], 1, i * part, part, 2 * rows, 2 * rows)
    half = rows // 2

    def cross(low):
        for h in (4, 5):
            sweep(visit.at[0], 0, h * rows + low, half)
            score(visit.at[2], 2, keep * part, part, h * rows + low, half)

            @pl.when(odd == 1)
            def _():
                score(visit.at[3], 5, keep * part, part, h * rows + low, half)
                score(visit.at[4], 6, keep * part, part, h * rows + low, half)

    for i in range(2):
        relay_x(i).wait_recv()

    @pl.when(odd == 1)
    def _():
        on_v().wait_recv()
        on_y().wait_recv()

    x_copy(2).wait_recv()
    relay_x(2).start()
    cross(0)

    @pl.when(odd == 1)
    def _():
        for i in range(keep):
            score(beside, 4, i * part, part, 0, 4 * rows)

    @pl.when(even)
    def _():
        for i in range(keep - 1):
            on_copy(i).wait_recv()
            score(visit.at[3], 4, i * part, part, 0, 4 * rows)

    x_copy(3).wait_recv()
    relay_x(3).start()

    @pl.when(odd == 1)
    def _():
        score(beside, 4, keep * part, part, 0, 4 * rows)

    @pl.when(even)
    def _():
        on_copy(keep - 1).wait_recv()
        score(visit.at[3], 4, (keep - 1) * part, part, 0, 4 * rows)

    for i in range(2, CHUNKS):
        relay_x(i).wait_recv()

    def col_copy(k):
        return send(col_acc.at[k], col_in.at[k], col_send.at[k], col_recv.at[k], owners[k])

    def row_copy(k):
        return send(row_out.at[k], row_in.at[k], row_send.at[k], row_recv.at[k],
                    row_owners[k + 1])

    def fold(h):
        return jnp.max(row_acc[h * rows:(h + 1) * rows, :].T.reshape(16, 8, rows), axis=0)

    for k in range(3):
        row_out[k] = fold(k + 1)
    col_copy(4).start()
    col_copy(1).start()
    for k in range(3):
        row_copy(k).start()
    cross(half)
    for k in range(3, 5):
        row_out[k] = fold(k + 1)
    col_copy(0).start()
    col_copy(2).start()

    @pl.when(odd == 1)
    def _():
        col_copy(5).start()
        col_copy(6).start()

    for k in range(3, 5):
        row_copy(k).start()
    early = fold(0)
    late = col_acc[3]
    for k in range(5):
        row_copy(k).wait_recv()
        early = jnp.maximum(early, row_in[k])
    for k in (4, 1, 0, 2):
        col_copy(k).wait_recv()
        late = jnp.maximum(late, col_in[k])

    @pl.when(odd == 1)
    def _():
        col_copy(5).wait_recv()
        col_copy(6).wait_recv()
        col_acc[3] = jnp.maximum(col_acc[3], jnp.maximum(col_in[5], col_in[6]))

    late = jnp.maximum(late, col_acc[3])
    early_ref[...] = jnp.max(early, axis=0, keepdims=True)
    late_ref[...] = jnp.max(late, axis=0, keepdims=True)

    core_copy().wait_send()
    for i in range(CHUNKS):
        z_copy(i).wait_send()
        y_copy(i).wait_send()
        x_copy(i).wait_send()
        relay_y(i).wait_send()
        relay_x(i).wait_send()
    for i in range(keep):
        side_copy(i).wait_send()
    up_copy().wait_send()

    @pl.when(even)
    def _():
        for i in range(keep):
            on_copy(i).wait_send()

    @pl.when(odd == 1)
    def _():
        on_v().wait_send()
        on_y().wait_send()
        col_copy(5).wait_send()
        col_copy(6).wait_send()

    for k in range(5):
        row_copy(k).wait_send()
    for k in (4, 1, 0, 2):
        col_copy(k).wait_send()


def shards(embeddings, ranks):
    rows, width = embeddings.shape
    copies = lax.axis_size("rep")
    blocks = lax.axis_size("blk")
    lines = ranks.reshape(-1, 128)
    dma = pltpu.SemaphoreType.DMA
    vmem = pl.BlockSpec(memory_space=pltpu.VMEM)
    early, late = pl.pallas_call(
        functools.partial(kernel, blocks, copies),
        out_shape=[jax.ShapeDtypeStruct((1, rows), jnp.float32)] * 2,
        in_specs=[pl.BlockSpec(memory_space=pltpu.HBM), vmem],
        out_specs=[vmem, vmem],
        scratch_shapes=[
            pltpu.VMEM((rows, width), jnp.float32),
            dma((CHUNKS,)),
            pltpu.VMEM((6 * rows, width), jnp.bfloat16),
            pltpu.VMEM((5, rows, width), jnp.bfloat16),
            pltpu.VMEM((6 * rows, 128), jnp.int32),
            pltpu.VMEM((7, 8, rows), jnp.int32),
            pltpu.VMEM((6 * rows, 128), jnp.float32),
            pltpu.VMEM((7, 8, rows), jnp.float32),
            pltpu.VMEM((7, 8, rows), jnp.float32),
            pltpu.VMEM((5, 8, rows), jnp.float32),
            pltpu.VMEM((5, 8, rows), jnp.float32),
            dma((CHUNKS,)), dma((CHUNKS,)), dma((CHUNKS,)), dma,
            dma((2, CHUNKS)), dma((CHUNKS,)), dma((CHUNKS + 1,)), dma((7,)), dma((5,)),
            dma((5, CHUNKS)), dma((CHUNKS,)), dma((CHUNKS,)), dma, dma((2, CHUNKS)), dma((7,)), dma((5,)),
        ],
        compiler_params=pltpu.CompilerParams(
            collective_id=0, has_side_effects=True, vmem_limit_bytes=63 * 1024 * 1024
        ),
    )(embeddings, lines)
    return early.reshape(rows), late.reshape(rows)


def solution(mesh):
    return jax.shard_map(
        shards,
        mesh=mesh,
        in_specs=(P(("blk", "rep"), None), P()),
        out_specs=(P(("blk", "rep")), P(("blk", "rep"))),
        check_vma=False,
    )
```
